32 devices in a mesh: gx: 32 (over z, y, x, core).
Axes of the slice: x: 2, y: 2, z: 4, core: 2. Of those that a mesh axis runs over, the one named last changes fastest.
Arguments:
- value: float32 [64, 48, 32, 128], P('gx'), may hold values from -6 to 6
- target: float32 [64, 48, 32, 128], P('gx'), may hold values from -6 to 6
- obstacle: float32 [64, 48, 32, 128], P('gx'), may hold values from -6 to -0.5
- fractions: float32 [16, 4], replicated, may hold values from 0 to 1
- control_cost: float32 [16], replicated, may hold values from 0 to 0.5
- shard_offset: int32 [16], replicated, may hold values from -8 to 8, as said below
- cell_offset: int32 [16], replicated, may hold values from 0 to 1
- grid_offset: int32 [16, 3], replicated, may hold values from -4 to 4
Outputs:
- updated: float32 [64, 48, 32, 128], P('gx')
The draws below stay inside these ranges and needn't reach their ends.
Inputs may be any that keep to these rules, and one draw needn't show every extreme that they name: `shard_offset`: every draw holds both -8 and 8.
All inputs are finite; a program needn't handle non-finite values.
Results may differ from the reference program's by a relative error of at most 0.00002.
Values sent between devices are 32-bit elements; how exact they have to be, the bound alone decides.
A program may use at most 128 MiB of HBM per device.

```python
import jax
import jax.numpy as jnp
from jax import lax

CX = 2
NY = 48
NZ = 32
NW = 128
NCTRL = 16
REACH = 8
NX = 64


def draw_shard_offset(key, part):
    first_key, second_key = jax.random.split(jax.random.fold_in(key, 11))
    offsets = jax.random.randint(first_key, (NCTRL,), -REACH, REACH + 1)
    order = jax.random.permutation(second_key, NCTRL)
    offsets = offsets.at[order[0]].set(-REACH).at[order[1]].set(REACH)
    return offsets.astype(jnp.int32)


def set_ends(entries, own_key, smallest, top_value):
    index_at = [jax.random.randint(jax.random.fold_in(own_key, axis), (), 0, length) for axis, length in enumerate(entries.shape)]
    widest = entries.shape.index(max(entries.shape))
    neighbour = index_at[:widest] + [(index_at[widest] + 1) % entries.shape[widest]] + index_at[widest + 1:]
    return entries.at[tuple(index_at)].set(smallest).at[tuple(neighbour)].set(top_value)


def block_levels(own_key, shape, cuts, low, high):
    def one(axis_at, blocks):
        heights = jax.random.uniform(jax.random.fold_in(jax.random.fold_in(own_key, 6), axis_at), (blocks,), jnp.float32, low / len(cuts), high / len(cuts))
        return jnp.repeat(jnp.exp(heights), shape[axis_at] // blocks).reshape((-1,) + (1,) * (len(shape) - axis_at - 1))

    level = one(*cuts[0])
    for cut in cuts[1:]:
        level = level * one(*cut)
    return level


def bell_draw(own_key, extent, width, reach, cuts=(), held_as=jnp.bfloat16):
    gain = block_levels(own_key, extent, cuts, -0.22, 0.18) if cuts else 1.0
    array = jax.random.normal(own_key, extent, jnp.float32) * width * gain
    return jnp.minimum(jnp.maximum(array, -reach), reach).astype(held_as)


def setup_inputs(seed: int = 0) -> dict:
    arg_keys = jax.random.split(jax.random.key(seed), 9)
    value = bell_draw(arg_keys[0], (NX, NY, NZ, NW), 1.0, 6.0, ((0, 32),), jnp.float32)
    target = bell_draw(arg_keys[1], (NX, NY, NZ, NW), 1.0, 6.0, ((0, 32),), jnp.float32)
    obstacle = jnp.clip(-6.0 + 5.5 * jax.random.uniform(arg_keys[2], (NX, NY, NZ, NW), jnp.float32) ** block_levels(arg_keys[2], (NX, NY, NZ, NW), ((0, 32),), -0.2, 0.2), -6.0, -0.5)
    fractions = jnp.clip(jax.random.uniform(arg_keys[3], (NCTRL, 4), jnp.float32, 0.0, 1.0), 0.0, 1.0)
    control_cost = jnp.clip(jax.random.uniform(arg_keys[4], (NCTRL,), jnp.float32, 0.0, 0.5), 0.0, 0.5)
    shard_offset = draw_shard_offset(jax.random.fold_in(arg_keys[8], 71), 0)
    cell_offset = set_ends(jax.random.randint(arg_keys[6], (NCTRL,), 0, CX), jax.random.fold_in(arg_keys[6], 1), 0, CX - 1).astype(jnp.int32)
    grid_offset = set_ends(jax.random.randint(arg_keys[7], (NCTRL, 3), -4, 5), jax.random.fold_in(arg_keys[7], 1), -4, 4).astype(jnp.int32)
    return {"value": value, "target": target, "obstacle": obstacle, "fractions": fractions, "control_cost": control_cost, "shard_offset": shard_offset, "cell_offset": cell_offset, "grid_offset": grid_offset}


def blend(low, high, frac):
    return (1.0 - frac) * low + frac * high


def reference(value, target, obstacle, fractions, control_cost, shard_offset, cell_offset, grid_offset):
    def one_control(u, best):
        along = (shard_offset[u] * CX + cell_offset[u]).astype(jnp.int32)
        field = blend(jnp.roll(value, -along, axis=0), jnp.roll(value, -along - 1, axis=0), fractions[u, 0])
        for axis_k in range(1, 4):
            moved = grid_offset[u, axis_k - 1].astype(jnp.int32)
            field = blend(jnp.roll(field, -moved, axis=axis_k), jnp.roll(field, -moved - 1, axis=axis_k), fractions[u, axis_k])
        return jnp.minimum(best, field + control_cost[u])

    start = jnp.full(value.shape, jnp.inf, jnp.float32)
    best = lax.fori_loop(0, NCTRL, one_control, start)
    return jnp.maximum(obstacle, jnp.minimum(target, best))
```

```python
import functools

import jax
import jax.numpy as jnp
from jax import lax
from jax.experimental import pallas as pl
from jax.experimental.pallas import tpu as pltpu
from jax.sharding import PartitionSpec as P

GROUP = 8
MESH = pl.DeviceIdType.MESH
CHUNK = 4
AHEAD = 3
REACH = 4
PAD = 8
TILE = 8
LAG = 2


def step_kernel(n, count, frac, cost, slab_at, cell_at, grid_at, value, own, low, high, *scratch):
    bufs = scratch[:count]
    mid, parts, send_sem, recv_sem, part_send, part_recv, own_sem = scratch[count:]
    rows, ny, nz, nw = value.shape
    controls = cost.shape[0]
    me = lax.axis_index("gx")
    j = lax.rem(me, GROUP)
    base = me - j
    core = lax.rem(j, 2)

    def xor(bits):
        got = j
        for bit in (1, 2, 4):
            if bits & bit:
                got = got + bit - 2 * bit * lax.rem(got // bit, 2)
        return got

    mate, xn, yn, diag = xor(1), xor(2), xor(4), xor(6)
    first, first_to = jnp.where(core == 0, xn, yn), jnp.where(core == 0, yn, xn)
    second = first_to
    down, up = lax.rem(me + n - GROUP, n), lax.rem(me + GROUP, n)

    barrier = pltpu.get_barrier_semaphore()
    for other in (base + mate, base + xn, base + yn, down, up):
        pl.semaphore_signal(barrier, inc=1, device_id=(other,), device_id_type=MESH)
    pl.semaphore_wait(barrier, 5)

    def source(q):
        return value.at[:, pl.ds((q * CHUNK - REACH) % ny, CHUNK)]

    def held(q, slot):
        return bufs[q].at[pl.ds(slot * rows, rows)]

    def copy(src, slot, kind, q, target):
        return pltpu.make_async_remote_copy(
            src_ref=src,
            dst_ref=held(q, slot),
            send_sem=send_sem.at[kind, q],
            recv_sem=recv_sem.at[slot, q],
            device_id=(target,),
            device_id_type=MESH,
        )

    def arrived(slot, q):
        ref = held(q, slot)
        pltpu.make_async_copy(ref, ref, recv_sem.at[slot, q]).wait()

    def to_halo(slot, src, q):
        @pl.when(jnp.logical_and(slot == 0, core == 0))
        def _():
            copy(src, GROUP, 7, q, down).start()

    def own_copy(q):
        return pltpu.make_async_copy(source(q), held(q, j), own_sem.at[q])

    def send_own(q):
        src = source(q)
        copy(src, j, 0, q, base + first).start()
        copy(src, j, 1, q, base + second).start()
        copy(src, j, 2, q, base + mate).start()
        to_halo(j, src, q)
        own_copy(q).start()

    def take(slot, q, kinds):
        arrived(slot, q)
        src = held(q, slot)
        for kind, target in kinds:
            copy(src, slot, kind, q, base + target).start()
        to_halo(slot, src, q)

    def place(u):
        return j + slab_at[u]

    def first_stage(q):
        buf = bufs[q]

        def one(u, c):
            at = place(u)
            at = jnp.where(at < 0, at + GROUP, at)
            at = jnp.where(at >= GROUP, at - GROUP, at)
            start = at * rows + cell_at[u]
            fx, fw = frac[u, 0], frac[u, 3]
            gw = grid_at[u, 2]
            turn = lax.rem(nw - gw, nw)
            turn1 = lax.rem(nw - gw - 1, nw)
            for y in range(CHUNK):
                below = buf[start, y]
                for r in range(rows):
                    above = buf[start + r + 1, y]
                    got = below + fx * (above - below)
                    left, right = pltpu.roll(got, turn, 1), pltpu.roll(got, turn1, 1)
                    got = left + fw * (right - left)
                    at_y = q * CHUNK + y
                    mid[u, r, at_y, PAD:PAD + nz] = got
                    mid[u, r, at_y, 0:PAD] = got[nz - PAD:]
                    mid[u, r, at_y, PAD + nz:2 * PAD + nz] = got[:PAD]
                    below = above
            return c

        lax.fori_loop(0, controls, one, 0, unroll=2)

    def second_stage(b):
        def tile(i, c):
            r, k = i // (nz // TILE), lax.rem(i, nz // TILE)

            def one(u, best):
                fy, fz, add = frac[u, 1], frac[u, 2], cost[u]
                gy, gz = grid_at[u, 0] + REACH, grid_at[u, 1]
                at = place(u)
                adds = (
                    jnp.where(at >= GROUP, add, jnp.inf),
                    jnp.where(at < 0, add, jnp.inf),
                    jnp.where(jnp.logical_and(at >= 0, at < GROUP), add, jnp.inf),
                )
                row = k * TILE + PAD + gz

                def along(y):
                    y_at = b * CHUNK + y + gy
                    if b * CHUNK + y + 2 * REACH >= ny:
                        y_at = jnp.where(y_at >= ny, y_at - ny, y_at)
                    left = mid[u, r, y_at, pl.ds(row, TILE)]
                    right = mid[u, r, y_at, pl.ds(row + 1, TILE)]
                    return left + fz * (right - left)

                new = []
                left = along(0)
                for y in range(CHUNK):
                    right = along(y + 1)
                    got = left + fy * (right - left)
                    new.append(tuple(jnp.minimum(best[y][s], got + adds[s]) for s in range(3)))
                    left = right
                return tuple(new)

            start = jnp.full((TILE, nw), jnp.inf, jnp.float32)
            best = lax.fori_loop(
                0, controls, one, tuple((start,) * 3 for _ in range(CHUNK)), unroll=4
            )
            ks = pl.ds(pl.multiple_of(k * TILE, TILE), TILE)
            for y in range(CHUNK):
                parts[0, r, b * CHUNK + y, ks] = best[y][0]
                parts[1, r, b * CHUNK + y, ks] = best[y][1]
                own[r, b * CHUNK + y, ks] = best[y][2]
            return c

        lax.fori_loop(0, rows * (nz // TILE), tile, 0)

    def part_copy(side, b):
        ys = pl.ds(b * CHUNK, CHUNK)
        return pltpu.make_async_remote_copy(
            src_ref=parts.at[side, :, ys],
            dst_ref=(high, low)[side].at[:, ys],
            send_sem=part_send.at[side, b],
            recv_sem=part_recv.at[side, b],
            device_id=((down, up)[side],),
            device_id_type=MESH,
        )

    def send_part(b):
        for side in range(2):
            part_copy(side, b).start()

    window = -(-(CHUNK + 2 * REACH + 1) // CHUNK) - 1
    done = 0
    sent = 0
    for q in range(min(AHEAD, count)):
        send_own(q)
    for s in range(count + LAG):
        ready = s - LAG
        if ready >= 0:

            @pl.when(core == 0)
            def _():
                arrived(GROUP, ready)
                copy(held(ready, GROUP), GROUP, 8, ready, base + mate).start()

        if s < count:
            take(first, s, [(3, first_to), (4, mate)])
            take(second, s, [(5, mate)])
            take(mate, s, [])
        if s + AHEAD < count:
            send_own(s + AHEAD)
        if 1 <= s <= count:
            take(diag, s - 1, [(6, mate)])
            take(xor(3), s - 1, [])
            take(xor(5), s - 1, [])
        if ready >= 0:
            take(xor(7), ready, [])

            @pl.when(core == 1)
            def _():
                arrived(GROUP, ready)

            own_copy(ready).wait()
            first_stage(ready)
            upto = count if ready == count - 1 else ready - window + 1
            while done < upto:
                second_stage(done)
                done += 1
                while sent < done - 1:
                    send_part(sent)
                    sent += 1
    for kind in range(9):
        for q in range(count):
            if kind < 7:
                copy(source(q), j, kind, q, base + mate).wait_send()
            elif kind == 8:

                @pl.when(core == 0)
                def _():
                    copy(source(q), j, kind, q, base + mate).wait_send()

            else:

                @pl.when(core == 0)
                def _():
                    copy(source(q), j, kind, q, base + mate).wait_send()

    while sent < count:
        send_part(sent)
        sent += 1
    for b in range(count):
        for side in range(2):
            part_copy(side, b).wait()


def step(n, value, frac, cost, slab_at, cell_at, grid_at):
    rows, ny, nz, nw = value.shape
    controls = cost.shape[0]
    count = ny // CHUNK
    smem = pl.BlockSpec(memory_space=pltpu.SMEM)
    vmem = pl.BlockSpec(memory_space=pltpu.VMEM)
    dma = pltpu.SemaphoreType.DMA
    return pl.pallas_call(
        functools.partial(step_kernel, n, count),
        out_shape=[pltpu.VMEM(value.shape, value.dtype)] * 3,
        in_specs=[smem] * 5 + [pl.BlockSpec(memory_space=pl.ANY)],
        out_specs=[vmem] * 3,
        scratch_shapes=[
            pltpu.VMEM(((GROUP + 1) * rows, CHUNK, nz, nw), value.dtype) for _ in range(count)
        ]
        + [
            pltpu.VMEM((controls, rows, ny, nz + 2 * PAD, nw), jnp.float32),
            pltpu.VMEM((2, rows, ny, nz, nw), jnp.float32),
            dma((9, count)),
            dma((GROUP + 1, count)),
            dma((2, count)),
            dma((2, count)),
            dma((count,)),
        ],
        compiler_params=pltpu.CompilerParams(
            collective_id=0, has_side_effects=True, vmem_limit_bytes=54 * 2**20
        ),
    )(frac, cost, slab_at, cell_at, grid_at, value)


def finish_kernel(target, obstacle, own, low, high, out):
    def one(y, c):
        for r in range(own.shape[0]):
            best = jnp.minimum(own[r, y], jnp.minimum(low[r, y], high[r, y]))
            out[r, y] = jnp.maximum(obstacle[r, y], jnp.minimum(target[r, y], best))
        return c

    lax.fori_loop(0, own.shape[1], one, 0, unroll=4)


def finish(target, obstacle, own, low, high):
    vmem = pl.BlockSpec(memory_space=pltpu.VMEM)
    return pl.pallas_call(
        finish_kernel,
        out_shape=jax.ShapeDtypeStruct(own.shape, own.dtype),
        in_specs=[vmem] * 5,
        out_specs=vmem,
        compiler_params=pltpu.CompilerParams(vmem_limit_bytes=20 * 2**20),
    )(target, obstacle, own, low, high)


def body(value, target, obstacle, *params):
    own, low, high = step(lax.axis_size("gx"), value, *params)
    return finish(target, obstacle, own, low, high)


def solution(mesh):
    slab = P("gx", None, None, None)
    return jax.shard_map(
        body,
        mesh=mesh,
        in_specs=(slab, slab, slab, P(), P(), P(), P(), P()),
        out_specs=slab,
        check_vma=False,
    )
```
